256 devices in a mesh: row: 8 (over x_hi, y), col: 32 (over x_lo, z, core).
Axes of the slice: x: 4 (x_hi: 2, x_lo: 2; x = x_hi * 2 + x_lo), y: 4, z: 8, core: 2. Of those that a mesh axis runs over, the one named last changes fastest.
Arguments:
- out_grad: bfloat16 [32768, 512], P('col', 'row'), may hold values from -6 to 6
- node_in: bfloat16 [32768, 512], P(('row', 'col')), may hold values from -0.03125 to 0.03125
- weights: bfloat16 [3, 512, 512], replicated, may hold values from -0.25 to 0.25
- tile_vals: bfloat16 [3, 32, 8, 32, 128, 128], P(None, 'col', 'row'), may hold values from -0.15625 to 0.15625
- tile_rows: int32 [3, 32, 8, 32], P(None, 'col', 'row'), may hold values from 0 to 7
- tile_cols: int32 [3, 32, 8, 32], P(None, 'col', 'row'), may hold values from 0 to 31
- tile_count: int32 [3, 32, 8], P(None, 'col', 'row'), may hold values from 1 to 32, as said below
Outputs:
- d_nodes: bfloat16 [32768, 512], P(('row', 'col'))
- d_weights: float32 [3, 512, 512], replicated
The draws below stay inside these ranges and needn't reach their ends.
Inputs may be any that keep to these rules, and one draw needn't show every extreme that they name: Only the first tile_count slots of a block's list hold tiles; later slots are ignored. In every relation some block uses all 32 slots. `tile_rows`: coordinates may repeat within a block's list; such tiles add.
All inputs are finite; a program needn't handle non-finite values.
Results may differ from the reference program's by a relative error of at most 0.005.
Values may be sent and summed in bfloat16 or wider, within the bound.
No kernel may reach another device: no remote copies, remote signals or barrier semaphores. Data moves between devices by JAX's collectives and lax.ppermute only.
A program may use at most 256 MiB of HBM per device.

```python
import jax
import jax.numpy as jnp
from jax import lax

D = 512
R = 3
TILE = 128
N_DEV = 128
CAP = 32
ROW_GROUPS = 8
COL_GROUPS = 32
NODES = 32768
TR = 8
TC = 32


def draw_tile_count(key, part):
    grid_shape = (R, COL_GROUPS, ROW_GROUPS)
    levels = jax.random.randint(jax.random.fold_in(key, 11), grid_shape, 1, 9)
    counts = jnp.maximum(1, CAP * levels * levels // 64)
    full_device = jax.random.randint(jax.random.fold_in(key, 12), (R,), 0, COL_GROUPS * ROW_GROUPS)
    flat_counts = counts.reshape(R, COL_GROUPS * ROW_GROUPS)
    chosen = jnp.arange(COL_GROUPS * ROW_GROUPS)[None, :] == full_device[:, None]
    flat_counts = jnp.where(chosen, CAP, flat_counts)
    return flat_counts.reshape(grid_shape).astype(jnp.int32)


def touch_ends(array, own_key, least, largest):
    extent = array.shape
    place = [jax.random.randint(jax.random.fold_in(own_key, axis), (), 0, extent[axis]) for axis in range(len(extent))]
    array = array.at[tuple(place)].set(least)
    longest = extent.index(max(extent))
    place[longest] = (place[longest] + 1) % extent[longest]
    return array.at[tuple(place)].set(largest)


def shard_levels(rng, shape, cuts, low, largest):
    def one(position, blocks):
        draws = jax.random.uniform(jax.random.fold_in(jax.random.fold_in(rng, 6), position), (blocks,), jnp.float32, low / len(cuts), largest / len(cuts))
        return jnp.repeat(jnp.exp(draws), shape[position] // blocks).reshape((-1,) + (1,) * (len(shape) - position - 1))

    loudness = one(*cuts[0])
    for cut in cuts[1:]:
        loudness = loudness * one(*cut)
    return loudness


def bell_draw(stream_key, dims, spread, most, split=(), held_as=jnp.bfloat16):
    drawn = spread * jax.random.normal(stream_key, dims, jnp.float32)
    if split:
        drawn = drawn * shard_levels(stream_key, dims, split, -0.22, 0.18)
    return jnp.clip(drawn, -most, most).astype(held_as)


def setup_inputs(seed: int = 0) -> dict:
    streams_of = jax.random.split(jax.random.key(seed), 8)
    out_grad = bell_draw(streams_of[0], (NODES, D), 1.0, 6.0, ((0, 32), (1, 8)))
    node_in = bell_draw(streams_of[1], (NODES, D), NODES ** -0.5, 0.03125, ((0, 256),))
    weights = bell_draw(streams_of[2], (R, D, D), D ** -0.5, 0.25)
    tile_vals = bell_draw(streams_of[3], (R, COL_GROUPS, ROW_GROUPS, CAP, TILE, TILE), (CAP * COL_GROUPS * 2 * TILE // (5 * TC)) ** -0.5, 0.15625, ((1, 32), (2, 8)))
    tile_rows = touch_ends(jax.random.randint(streams_of[4], (R, COL_GROUPS, ROW_GROUPS, CAP), 0, TR), jax.random.fold_in(streams_of[4], 1), 0, TR - 1).astype(jnp.int32)
    tile_cols = touch_ends(jax.random.randint(streams_of[5], (R, COL_GROUPS, ROW_GROUPS, CAP), 0, TC), jax.random.fold_in(streams_of[5], 1), 0, TC - 1).astype(jnp.int32)
    tile_count = draw_tile_count(jax.random.fold_in(streams_of[7], 71), 0)
    return {"out_grad": out_grad, "node_in": node_in, "weights": weights, "tile_vals": tile_vals, "tile_rows": tile_rows, "tile_cols": tile_cols, "tile_count": tile_count}


def block_products(operand, tile_block, row_ids, col_ids, count_now, block_index):
    group_col = block_index // ROW_GROUPS
    group_row = block_index % ROW_GROUPS
    lanes = jnp.arange(TILE, dtype=jnp.int32)
    source_ids = (group_col * (N_DEV * ROW_GROUPS) + row_ids[:, None] * TILE + lanes[None, :]).astype(jnp.int32)
    sources = jnp.take(operand, source_ids.reshape(-1), axis=0).reshape(CAP, TILE, 2 * D)
    live = (jnp.arange(CAP, dtype=jnp.int32) < count_now).astype(jnp.float32)
    products = jnp.einsum("skt,skd->std", tile_block.astype(jnp.float32), sources.astype(jnp.float32), precision=lax.Precision.HIGHEST)
    products = products * live[:, None, None]
    target_ids = (group_row * (N_DEV * COL_GROUPS) + col_ids[:, None] * TILE + lanes[None, :]).astype(jnp.int32)
    return target_ids.reshape(-1), products.reshape(CAP * TILE, 2 * D)


def reference(out_grad, node_in, weights, tile_vals, tile_rows, tile_cols, tile_count):
    blocks = COL_GROUPS * ROW_GROUPS
    block_ids = jnp.arange(blocks, dtype=jnp.int32)
    mixed_total = jnp.zeros((NODES, D), jnp.float32)
    weight_grads = []
    inputs_wide = node_in.astype(jnp.float32)
    for relation in range(R):
        premixed = jnp.dot(out_grad, weights[relation].T, preferred_element_type=jnp.float32).astype(jnp.bfloat16)
        operand = jnp.concatenate([out_grad, premixed], axis=1)

        def block_step(summed, inputs):
            target_ids, products = block_products(operand, inputs[0], inputs[1], inputs[2], inputs[3], inputs[4])
            return summed.at[target_ids].add(products), None

        scanned = (tile_vals[relation].reshape(blocks, CAP, TILE, TILE), tile_rows[relation].reshape(blocks, CAP), tile_cols[relation].reshape(blocks, CAP), tile_count[relation].reshape(blocks), block_ids)
        start_sums = jnp.zeros((NODES, 2 * D), jnp.float32)
        summed, ignored = lax.scan(block_step, start_sums, scanned)
        weight_grads.append(jnp.dot(inputs_wide.T, summed[:, :D], precision=lax.Precision.HIGHEST))
        mixed_total = mixed_total + summed[:, D:]
    return mixed_total.astype(jnp.bfloat16), jnp.stack(weight_grads)
```

```python
import functools

import jax
import jax.numpy as jnp
from jax import lax
from jax.experimental import pallas as pl
from jax.experimental.pallas import tpu as pltpu
from jax.sharding import Mesh
from jax.sharding import PartitionSpec as P

XHI, Y, XLO, Z, CORE = "row_0", "row_1", "col_0", "col_1", "col_2"
ROW = (XHI, Y)
COL = (XLO, Z, CORE)
X4 = (XHI, XLO)

UNROLL = 4
F32 = jnp.float32
BF16 = jnp.bfloat16


def shifted(value, axis, step):
    n = lax.axis_size(axis)
    return lax.ppermute(value, axis, [(i, (i + step) % n) for i in range(n)])


def slots(count, body):
    def group(g, carry):
        body([g * UNROLL + u for u in range(UNROLL)])
        return carry

    lax.fori_loop(0, (count + UNROLL - 1) // UNROLL, group, 0)


def mix_kernel(place, rows, cols, counts, g0, g1, g2, g3, weights, tiles, out, grad, pieces, premixed, acc):
    x_hi, y, x_lo, z, core = [place[i] for i in range(5)]
    relations = weights.shape[0]
    half = pieces.shape[1]
    for k, block in enumerate((g0, g1, g2, g3)):
        for a in range(2):
            pieces[(x_hi ^ a) * 4 + ((y - k) & 3)] = block[a]
    for j in range(4):
        left, right = pieces[2 * j], pieces[2 * j + 1]
        lanes = slice(128 * j, 128 * (j + 1))
        grad[:half, lanes] = jnp.concatenate([left[:, :64], right[:, :64]], axis=1)
        grad[half:, lanes] = jnp.concatenate([left[:, 64:], right[:, 64:]], axis=1)
    acc[...] = jnp.zeros_like(acc)
    for r in range(relations):
        mixed = lax.dot_general(
            weights[r], grad[...], (((1,), (1,)), ((), ())), preferred_element_type=F32
        ).astype(BF16)
        for k in range(premixed.shape[0]):
            premixed[k] = mixed[:, 128 * k : 128 * (k + 1)]
        count = counts[r]

        def group(ids, r=r, count=count):
            products = []
            for s in ids:
                tile = tiles[r, s]
                tile = jnp.where(s < count, tile, jnp.zeros_like(tile))
                products.append(jnp.dot(premixed[rows[r, s]], tile, preferred_element_type=F32))
            for s, product in zip(ids, products):
                c = cols[r, s]
                at = ((c & 1) ^ core) * 16 + ((c >> 4) ^ x_lo) * 8 + (((c >> 1) - z) & 7)
                acc[at] += product

        slots(count, group)
    out[...] = acc[...].astype(BF16)


def weight_kernel(place, rows, cols, counts, own, other, grad, tiles, out, sums, held):
    x_hi, y, x_lo, z, core = [place[i] for i in range(5)]
    x = x_hi * 2 + x_lo
    relations = tiles.shape[0]
    for r in range(relations):
        sums[...] = jnp.zeros_like(sums)
        count = counts[r]

        def group(ids, r=r, count=count):
            products = []
            for s in ids:
                tile = tiles[r, s]
                tile = jnp.where(s < count, tile, jnp.zeros_like(tile))
                c = cols[r, s]
                at = ((c >> 1) & 7) * 2 + ((c >> 4) ^ x_lo)
                inputs = jnp.where((c & 1) == core, own[at], other[at])
                products.append(
                    lax.dot_general(inputs, tile, (((1,), (1,)), ((), ())), preferred_element_type=F32)
                )
            for s, product in zip(ids, products):
                sums[rows[r, s]] += product

        slots(count, group)
        for k in range(sums.shape[0]):
            held[:, 128 * k : 128 * (k + 1)] = sums[k].astype(BF16)
        terms = jnp.dot(held[...], grad[...], preferred_element_type=F32)
        for h in range(2):
            for yb in range(4):
                for xb in range(4):
                    d = (h * 16 + yb * 4 + xb) * 16
                    out[h ^ core, (yb - y) & 3, (xb - x) & 3, r] = terms[d : d + 16]


def join_kernel(place, own, other, out):
    x_hi, y, x_lo, z, core = [place[i] for i in range(5)]
    x = x_hi * 2 + x_lo
    for a, block in enumerate((own, other)):
        for ky in range(4):
            for kx in range(4):
                d = ((core ^ a) * 16 + ((y - ky) & 3) * 4 + ((x - kx) & 3)) * 16
                for r in range(out.shape[0]):
                    out[r, pl.ds(pl.multiple_of(d, 16), 16), :] = block[ky, kx, r].astype(F32)


SMEM = pl.BlockSpec(memory_space=pltpu.SMEM)
VMEM = pl.BlockSpec(memory_space=pltpu.VMEM)


def added(first, *others):
    total = first.astype(F32)
    for other in others:
        total = total + other.astype(F32)
    return total


def body(out_grad, node_in, weights, tile_vals, tile_rows, tile_cols, tile_count):
    place = jnp.stack([lax.axis_index(a) for a in (XHI, Y, XLO, Z, CORE)]).astype(jnp.int32)
    relations, d_in, d_out = weights.shape
    tiles, rows, cols, counts = tile_vals[:, 0, 0], tile_rows[:, 0, 0], tile_cols[:, 0, 0], tile_count[:, 0, 0]
    half = out_grad.shape[0] // 2

    packed = jnp.concatenate([out_grad[:half], out_grad[half:]], axis=1)
    pair = jnp.stack([packed, shifted(packed, XHI, 1)])
    grads = [pair] + [shifted(pair, Y, k) for k in (1, 2, 3)]

    turned = node_in.T
    inputs = jnp.stack([turned, shifted(turned, XLO, 1)])
    inputs = lax.all_gather(inputs, Z).reshape(16, d_in, 128)
    inputs_other = shifted(inputs, CORE, 1)

    partial, grad = pl.pallas_call(
        mix_kernel,
        out_shape=(
            jax.ShapeDtypeStruct((32, d_in, 128), BF16),
            jax.ShapeDtypeStruct((2 * half, d_out), BF16),
        ),
        in_specs=[SMEM] * 4 + [VMEM] * 6,
        out_specs=(VMEM, VMEM),
        scratch_shapes=[
            pltpu.VMEM((8, half, 128), BF16),
            pltpu.VMEM((8, d_in, 128), BF16),
            pltpu.VMEM((32, d_in, 128), F32),
        ],
        compiler_params=pltpu.CompilerParams(vmem_limit_bytes=48 * 2**20),
        name="mix",
    )(place, rows, cols, counts, *grads, weights, tiles)

    terms = pl.pallas_call(
        weight_kernel,
        out_shape=jax.ShapeDtypeStruct((2, 4, 4, relations, 16, d_out), F32),
        in_specs=[SMEM] * 4 + [VMEM] * 4,
        out_specs=VMEM,
        scratch_shapes=[
            pltpu.VMEM((8, d_in, 128), F32),
            pltpu.VMEM((d_in, 2 * half), BF16),
        ],
        compiler_params=pltpu.CompilerParams(vmem_limit_bytes=48 * 2**20),
        name="weight_terms",
    )(place, rows, cols, counts, inputs, inputs_other, grad, tiles)

    met = added(partial[:16], shifted(partial[16:], CORE, 1))
    crossed = []
    for k in (0, 4):
        crossed.append(added(met[k : k + 4], shifted(met[8 + k : 12 + k].astype(BF16), XLO, 1)))
    crossed = [c[i] for c in crossed for i in range(4)]
    total = added(crossed[0], *[shifted(crossed[k].astype(BF16), Z, k) for k in range(1, 8)])
    d_nodes = total.astype(BF16).T

    met = added(terms[0], shifted(terms[1], CORE, 1))
    met = added(met[0], *[shifted(met[k].astype(BF16), Y, k) for k in (1, 2, 3)])
    met = added(met[0], *[shifted(met[k].astype(BF16), X4, k) for k in (1, 2, 3)])
    spread = jnp.broadcast_to(met.astype(BF16)[None], (8, *met.shape))
    met = lax.all_to_all(spread, Z, 0, 0)
    met = added(*[met[k] for k in range(8)]).astype(BF16)
    met = jnp.stack([met] + [shifted(met, X4, k) for k in (1, 2, 3)])
    met = jnp.stack([met] + [shifted(met, Y, k) for k in (1, 2, 3)])
    d_weights = pl.pallas_call(
        join_kernel,
        out_shape=jax.ShapeDtypeStruct((relations, d_in, d_out), F32),
        in_specs=[SMEM, VMEM, VMEM],
        out_specs=VMEM,
        name="join",
    )(place, met, shifted(met, CORE, 1))
    return d_nodes, d_weights


def solution(mesh):
    finer = Mesh(mesh.devices.reshape(2, 4, 2, 8, 2), (XHI, Y, XLO, Z, CORE))
    in_specs = (
        P(COL, ROW),
        P(ROW + COL, None),
        P(),
        P(None, COL, ROW, None, None, None),
        P(None, COL, ROW, None),
        P(None, COL, ROW, None),
        P(None, COL, ROW),
    )
    out_specs = (P(ROW + COL, None), P())
    return jax.shard_map(body, mesh=finer, in_specs=in_specs, out_specs=out_specs, check_vma=False)
```

```python
import jax
import jax.numpy as jnp
from jax import lax
from jax.experimental import pallas as pl
from jax.experimental.pallas import tpu as pltpu
from jax.sharding import Mesh
from jax.sharding import PartitionSpec as P


XHI, Y, XLO, Z, CORE = "row_0", "row_1", "col_0", "col_1", "col_2"
ROW = (XHI, Y)
COL = (XLO, Z, CORE)
NEAR = (XLO, Z)
X4 = (XHI, XLO)

UNROLL = 4
CAP = 32
TILE = 128
F32 = jnp.float32
BF16 = jnp.bfloat16
SMEM = pl.BlockSpec(memory_space=pltpu.SMEM)
VMEM = pl.BlockSpec(memory_space=pltpu.VMEM)
ANY = pl.BlockSpec(memory_space=pltpu.HBM)
BUSY = pl.CostEstimate(flops=40 * 10**9, transcendentals=0, bytes_accessed=2**23)
ROOMY = pltpu.CompilerParams(vmem_limit_bytes=24 * 2**20)
SMALL = pltpu.CompilerParams(vmem_limit_bytes=8 * 2**20)


def shifted(value, axis, step):
    n = lax.axis_size(axis)
    return lax.ppermute(value, axis, [(i, (i + step) % n) for i in range(n)])


def around(value, axis):
    n = lax.axis_size(axis)
    held = {0: value}
    for step in range(1, n // 2 + 1):
        held[step] = shifted(held[step - 1], axis, 1)
        if n - step > step:
            held[n - step] = shifted(held[(n - step + 1) % n], axis, -1)
    return [held[k] for k in range(n)]


def swapped(value, axis, step):
    return lax.ppermute(value, axis, [(i, i ^ step) for i in range(lax.axis_size(axis))])


def added(first, *others):
    total = first.astype(F32)
    for other in others:
        total = total + other.astype(F32)
    return total


def columns(core, meta, r, picked, body):
    count = meta[r, 2 * CAP]

    def pick(s, n):
        picked[n] = s
        return n + jnp.where((meta[r, CAP + s] & 1) == core, 1, 0)

    found = lax.fori_loop(0, count, pick, 0)
    for u in range(UNROLL):
        picked[found + u] = 0

    def group(g, carry):
        at = [g * UNROLL + u for u in range(UNROLL)]
        ids = [picked[i] for i in at]
        body([(s, i < found, meta[r, s], meta[r, CAP + s]) for i, s in zip(at, ids)])
        return carry

    lax.fori_loop(0, (found + UNROLL - 1) // UNROLL, group, 0)


def fetches(tiles0, tiles1, tiles, arrived):
    return lambda a, r: pltpu.make_async_copy((tiles0, tiles1)[a].at[r], tiles.at[a, r], arrived.at[a, r])


def masked(tile, keep):
    return jnp.where(keep, tile, jnp.zeros_like(tile))


def prepare_kernel(node_in, rows, cols, counts, turned, meta):
    turned[...] = node_in[...].astype(F32).T.astype(BF16)
    for r in range(meta.shape[0]):
        meta[r : r + 1, :CAP] = rows[r, 0]
        meta[r : r + 1, CAP : 2 * CAP] = cols[r, 0]
        meta[r : r + 1, 2 * CAP :] = jnp.full((1, meta.shape[1] - 2 * CAP), counts[r, 0, 0], jnp.int32)


def grad_kernel(g0, g1, g2, g3, grad):
    x_hi, y = lax.axis_index(XHI), lax.axis_index(Y)
    for k, block in enumerate((g0, g1, g2, g3)):
        for a in range(2):
            grad[(x_hi ^ a) * 4 + ((y - k) & 3)] = block[a]


def mix_kernel(meta0, meta1, grad0, grad1, weights, tiles0, tiles1, out, picked, premixed, acc, held_tiles, arrived):
    core = lax.axis_index(CORE)
    fetch = fetches(tiles0, tiles1, held_tiles, arrived)
    for r in range(weights.shape[0]):
        for a in range(2):
            fetch(a, r).start()
    acc[...] = jnp.zeros_like(acc)

    def relation(r, carry):
        for a, (meta, grad) in enumerate(((meta0, grad0), (meta1, grad1))):
            mixed = lax.dot_general(
                weights[r], grad[...], (((1,), (0,)), ((), ())), preferred_element_type=F32
            ).astype(BF16)
            for k in range(premixed.shape[0]):
                premixed[k] = mixed[:, TILE * k : TILE * (k + 1)]

            fetch(a, r).wait()

            def group(entries, a=a):
                products = [
                    jnp.dot(premixed[row], masked(held_tiles[a, r, s], keep), preferred_element_type=F32)
                    for s, keep, row, col in entries
                ]
                for (s, keep, row, col), product in zip(entries, products):
                    acc[col >> 1] += product

            columns(core, meta, r, picked, group)
        return carry

    lax.fori_loop(0, weights.shape[0], relation, 0)
    out[...] = acc[...].astype(BF16)


def weight_kernel(meta0, meta1, *refs):
    parts = refs[:8]
    grad0, grad1, tiles0, tiles1, kept, sent, picked, inputs, sums, held, held_tiles, arrived = refs[8:]
    core, x_hi, y, x_lo, z = [lax.axis_index(a) for a in (CORE, XHI, Y, XLO, Z)]
    fetch = fetches(tiles0, tiles1, held_tiles, arrived)
    for r in range(tiles0.shape[0]):
        for a in range(2):
            fetch(a, r).start()
    x = x_hi * 2 + x_lo
    for k, part in enumerate(parts):
        inputs[2 * k] = part[0]
        inputs[2 * k + 1] = part[1]

    def relation(r, carry):
        terms = None
        for a, (meta, grad) in enumerate(((meta0, grad0), (meta1, grad1))):
            fetch(a, r).wait()
            sums[...] = jnp.zeros_like(sums)

            def group(entries, a=a):
                products = [
                    lax.dot_general(
                        inputs[((z - (col >> 1)) & 7) * 2 + ((col >> 4) ^ x_lo)],
                        masked(held_tiles[a, r, s], keep),
                        (((1,), (1,)), ((), ())),
                        preferred_element_type=F32,
                    )
                    for s, keep, row, col in entries
                ]
                for (s, keep, row, col), product in zip(entries, products):
                    sums[row] += product

            columns(core, meta, r, picked, group)
            for k in range(sums.shape[0]):
                held[:, TILE * k : TILE * (k + 1)] = sums[k].astype(BF16)
            part = lax.dot_general(
                held[...], grad[...], (((1,), (1,)), ((), ())), preferred_element_type=F32
            )
            terms = part if terms is None else terms + part
        half = terms.shape[0] // 2
        low, high = terms[:half], terms[half:]
        mine = jnp.where(core == 0, low, high)
        theirs = jnp.where(core == 0, high, low).astype(BF16)
        for yb in range(4):
            for xb in range(4):
                d = (yb * 4 + xb) * 16
                kept[(yb - y) & 3, (xb - x) & 3, r] = mine[d : d + 16]
                sent[(yb - y) & 3, (xb - x) & 3, r] = theirs[d : d + 16]
        return carry

    lax.fori_loop(0, tiles0.shape[0], relation, 0)


def nodes_kernel(parts, out):
    total = parts[0].astype(F32)
    for k in range(1, parts.shape[0]):
        total += parts[k].astype(F32)
    out[...] = total.T.astype(BF16)


def join_kernel(own, other, out):
    core, x_hi, y, x_lo = [lax.axis_index(a) for a in (CORE, XHI, Y, XLO)]
    x = x_hi * 2 + x_lo
    for a, block in enumerate((own, other)):
        for ky in range(4):
            for kx in range(4):
                d = ((core ^ a) * 16 + ((y - ky) & 3) * 4 + ((x - kx) & 3)) * 16
                out[0, pl.ds(pl.multiple_of(d, 16), 16), :] = block[ky, kx, 0].astype(F32)


def body(out_grad, node_in, weights, tile_vals, tile_rows, tile_cols, tile_count):
    relations, d_in, d_out = weights.shape
    tiles = tile_vals[:, 0, 0]
    rows, width = out_grad.shape

    turned, meta = pl.pallas_call(
        prepare_kernel,
        out_shape=(
            jax.ShapeDtypeStruct((d_in, TILE), BF16),
            jax.ShapeDtypeStruct((relations, TILE), jnp.int32),
        ),
        in_specs=[VMEM] * 3 + [SMEM],
        out_specs=(VMEM, VMEM),
        compiler_params=SMALL,
        name="prepare",
    )(node_in, tile_rows, tile_cols, tile_count)
    packed = out_grad.T
    pair = jnp.stack([packed, shifted(packed, XHI, 1)])
    grads = [pair] + [shifted(pair, Y, k) for k in (1, 2, 3)]
    parts = around(jnp.stack([turned, shifted(turned, XLO, 1)]), Z)
    tiles_near = shifted(tiles, CORE, 1)
    meta_near = shifted(meta, CORE, 1)

    grad = pl.pallas_call(
        grad_kernel,
        out_shape=jax.ShapeDtypeStruct((d_out // width, width, rows), BF16),
        in_specs=[VMEM] * 4,
        out_specs=VMEM,
        compiler_params=SMALL,
        name="join_grad",
    )(*grads).reshape(d_out, rows)
    grad_near = shifted(grad, CORE, 1)

    partial = pl.pallas_call(
        mix_kernel,
        out_shape=jax.ShapeDtypeStruct((16, d_in, TILE), BF16),
        in_specs=[SMEM] * 2 + [VMEM] * 3 + [ANY] * 2,
        out_specs=VMEM,
        scratch_shapes=[
            pltpu.SMEM((CAP + UNROLL,), jnp.int32),
            pltpu.VMEM((8, d_in, TILE), BF16),
            pltpu.VMEM((16, d_in, TILE), F32),
            pltpu.VMEM((2, *tiles.shape), BF16),
            pltpu.SemaphoreType.DMA((2, relations)),
        ],
        compiler_params=ROOMY,
        cost_estimate=BUSY,
        name="mix",
    )(meta, meta_near, grad, grad_near, weights, tiles, tiles_near)
    mixed = lax.all_to_all(partial, NEAR, 0, 0)
    d_nodes = pl.pallas_call(
        nodes_kernel,
        out_shape=jax.ShapeDtypeStruct(node_in.shape, BF16),
        in_specs=[VMEM],
        out_specs=VMEM,
        compiler_params=SMALL,
        name="nodes",
    )(mixed)

    kept, sent = pl.pallas_call(
        weight_kernel,
        out_shape=(
            jax.ShapeDtypeStruct((4, 4, relations, 16, d_out), F32),
            jax.ShapeDtypeStruct((4, 4, relations, 16, d_out), BF16),
        ),
        in_specs=[SMEM] * 2 + [VMEM] * 10 + [ANY] * 2,
        out_specs=(VMEM, VMEM),
        scratch_shapes=[
            pltpu.SMEM((CAP + UNROLL,), jnp.int32),
            pltpu.VMEM((16, d_in, TILE), BF16),
            pltpu.VMEM((8, d_in, TILE), F32),
            pltpu.VMEM((d_in, rows), BF16),
            pltpu.VMEM((2, *tiles.shape), BF16),
            pltpu.SemaphoreType.DMA((2, relations)),
        ],
        compiler_params=ROOMY,
        cost_estimate=BUSY,
        name="weight_terms",
    )(meta, meta_near, *parts, grad, grad_near, tiles, tiles_near)

    met = shifted(sent, CORE, 1)
    on_y = [added(kept[k], met[k]) for k in range(4)]
    on_y = added(on_y[0], *[shifted(on_y[k].astype(BF16), Y, k) for k in (1, 2, 3)])
    on_x = added(on_y[0], *[shifted(on_y[k].astype(BF16), X4, k) for k in (1, 2, 3)])
    on_z = (on_x + swapped(on_x, Z, 1)).astype(BF16)
    by = [on_z] + [shifted(on_z, Z, k) for k in (2, 4, 6)]
    total = (added(by[0], by[2]) + added(by[1], by[3])).astype(BF16)
    total = jnp.stack([total] + [shifted(total, X4, k) for k in (1, 2, 3)])
    total = jnp.stack([total] + [shifted(total, Y, k) for k in (1, 2, 3)])
    share = pl.BlockSpec((4, 4, 1, 16, d_out), lambda r: (0, 0, r, 0, 0))
    d_weights = pl.pallas_call(
        join_kernel,
        out_shape=jax.ShapeDtypeStruct((relations, d_in, d_out), F32),
        grid=(relations,),
        in_specs=[share, share],
        out_specs=pl.BlockSpec((1, d_in, d_out), lambda r: (r, 0, 0)),
        compiler_params=SMALL,
        name="join",
    )(total, shifted(total, CORE, 1))
    return d_nodes, d_weights


def solution(mesh):
    finer = Mesh(mesh.devices.reshape(2, 4, 2, 8, 2), (XHI, Y, XLO, Z, CORE))
    in_specs = (
        P(COL, ROW),
        P(ROW + COL, None),
        P(),
        P(None, COL, ROW, None, None, None),
        P(None, COL, ROW, None),
        P(None, COL, ROW, None),
        P(None, COL, ROW),
    )
    out_specs = (P(ROW + COL, None), P())
    return jax.shard_map(body, mesh=finer, in_specs=in_specs, out_specs=out_specs, check_vma=False)
```

```python
import jax
import jax.numpy as jnp
from jax import lax
from jax.experimental import pallas as pl
from jax.experimental.pallas import tpu as pltpu
from jax.sharding import Mesh
from jax.sharding import PartitionSpec as P


XHI, Y, XLO, Z, CORE = "row_0", "row_1", "col_0", "col_1", "col_2"
ROW = (XHI, Y)
COL = (XLO, Z, CORE)
X4 = (XHI, XLO)

UNROLL = 4
CAP = 32
TILE = 128
F32 = jnp.float32
BF16 = jnp.bfloat16
SMEM = pl.BlockSpec(memory_space=pltpu.SMEM)
VMEM = pl.BlockSpec(memory_space=pltpu.VMEM)
ANY = pl.BlockSpec(memory_space=pltpu.HBM)
BUSY = pl.CostEstimate(flops=40 * 10**9, transcendentals=0, bytes_accessed=2**23)
SMALL = pltpu.CompilerParams(vmem_limit_bytes=8 * 2**20)


def shifted(value, axis, step):
    n = lax.axis_size(axis)
    return lax.ppermute(value, axis, [(i, (i + step) % n) for i in range(n)])


def gathered(value, axes):
    copies = jnp.broadcast_to(value[None], (lax.axis_size(axes), *value.shape))
    return lax.all_to_all(copies, axes, 0, 0)


def swapped(value, axis, step):
    return lax.ppermute(value, axis, [(i, i ^ step) for i in range(lax.axis_size(axis))])


def added(first, *others):
    total = first.astype(F32)
    for other in others:
        total = total + other.astype(F32)
    return total


def columns(core, meta, r, picked, body):
    count = meta[r, 2 * CAP]

    def pick(s, n):
        picked[n] = s
        return n + jnp.where((meta[r, CAP + s] & 1) == core, 1, 0)

    found = lax.fori_loop(0, count, pick, 0)
    for u in range(UNROLL):
        picked[found + u] = 0

    def group(g, carry):
        at = [g * UNROLL + u for u in range(UNROLL)]
        ids = [picked[i] for i in at]
        body([(s, i < found, meta[r, s], meta[r, CAP + s]) for i, s in zip(at, ids)])
        return carry

    lax.fori_loop(0, (found + UNROLL - 1) // UNROLL, group, 0)


def fetches(tiles0, tiles1, tiles, arrived):
    return lambda a, r: pltpu.make_async_copy((tiles0, tiles1)[a].at[r], tiles.at[a, r], arrived.at[a, r])


def masked(tile, keep):
    return jnp.where(keep, tile, jnp.zeros_like(tile))


def turn_kernel(node_in, turned):
    turned[...] = node_in[...].astype(F32).T.astype(BF16)


def meta_kernel(rows, cols, counts, meta):
    for r in range(meta.shape[0]):
        meta[r : r + 1, :CAP] = rows[r, 0]
        meta[r : r + 1, CAP : 2 * CAP] = cols[r, 0]
        meta[r : r + 1, 2 * CAP :] = jnp.full((1, meta.shape[1] - 2 * CAP), counts[r], jnp.int32)


def grad_kernel(g0, g1, g2, g3, grad):
    x_hi, y = lax.axis_index(XHI), lax.axis_index(Y)
    for k, block in enumerate((g0, g1, g2, g3)):
        for a in range(2):
            grad[(x_hi ^ a) * 4 + ((y - k) & 3)] = block[a]


def mix_kernel(
    meta0, meta1, grad0, grad1, weights, tiles0, tiles1,
    kept, sent, sums, picked, operands, mixed_acc, own_acc, held_tiles, arrived,
):
    core, x_lo = lax.axis_index(CORE), lax.axis_index(XLO)
    fetch = fetches(tiles0, tiles1, held_tiles, arrived)
    for r in range(weights.shape[0]):
        for a in range(2):
            fetch(a, r).start()
    d_in = weights.shape[1]
    mixed_acc[...] = jnp.zeros_like(mixed_acc)
    for a, grad in enumerate((grad0, grad1)):
        for k in range(operands.shape[1]):
            operands[a, k, d_in:] = grad[:, TILE * k : TILE * (k + 1)]

    def relation(r, carry):
        own_acc[...] = jnp.zeros_like(own_acc)
        for a, (meta, grad) in enumerate(((meta0, grad0), (meta1, grad1))):
            mixed = jnp.dot(weights[r], grad[...], preferred_element_type=F32).astype(BF16)
            for k in range(operands.shape[1]):
                operands[a, k, :d_in] = mixed[:, TILE * k : TILE * (k + 1)]
            fetch(a, r).wait()

            def group(entries, a=a):
                products = [
                    jnp.dot(operands[a, row], masked(held_tiles[a, r, s], keep), preferred_element_type=F32)
                    for s, keep, row, col in entries
                ]
                for (s, keep, row, col), product in zip(entries, products):
                    mixed_acc[((col >> 4) ^ x_lo) * 8 + ((col >> 1) & 7)] += product[:d_in]
                    own_acc[col >> 1] += product[d_in:]

            columns(core, meta, r, picked, group)
        for k in range(own_acc.shape[0]):
            sums[r, :, TILE * k : TILE * (k + 1)] = own_acc[k].astype(BF16)
        return carry

    lax.fori_loop(0, weights.shape[0], relation, 0)
    kept[...] = mixed_acc[:8].astype(BF16)
    sent[...] = mixed_acc[8:].astype(BF16)


def weight_kernel(inputs, sums, kept, sent, held):
    core, x_hi, y, x_lo = [lax.axis_index(a) for a in (CORE, XHI, Y, XLO)]
    x = x_hi * 2 + x_lo
    for k in range(inputs.shape[0]):
        held[:, TILE * k : TILE * (k + 1)] = inputs[k]
    for r in range(sums.shape[0]):
        terms = lax.dot_general(held[...], sums[r], (((1,), (1,)), ((), ())), preferred_element_type=F32)
        half = terms.shape[0] // 2
        low, high = terms[:half], terms[half:]
        mine = jnp.where(core == 0, low, high)
        theirs = jnp.where(core == 0, high, low).astype(BF16)
        for yb in range(4):
            for xb in range(4):
                d = (yb * 4 + xb) * 16
                kept[(yb - y) & 3, (xb - x) & 3, r] = mine[d : d + 16]
                sent[(yb - y) & 3, (xb - x) & 3, r] = theirs[d : d + 16]


def nodes_kernel(parts, out):
    total = parts[0].astype(F32)
    for k in range(1, parts.shape[0]):
        total += parts[k].astype(F32)
    out[...] = total.T.astype(BF16)


def join_kernel(own, other, out):
    core, x_hi, y, x_lo = [lax.axis_index(a) for a in (CORE, XHI, Y, XLO)]
    x = x_hi * 2 + x_lo
    for a, block in enumerate((own, other)):
        for ky in range(4):
            for kx in range(4):
                d = ((core ^ a) * 16 + ((y - ky) & 3) * 4 + ((x - kx) & 3)) * 16
                out[0, pl.ds(pl.multiple_of(d, 16), 16), :] = block[ky, kx, 0].astype(F32)


def body(out_grad, node_in, weights, tile_vals, tile_rows, tile_cols, tile_count):
    relations, d_in, d_out = weights.shape
    tiles = tile_vals[:, 0, 0]
    rows, width = out_grad.shape

    turned = pl.pallas_call(
        turn_kernel,
        out_shape=jax.ShapeDtypeStruct((d_in, TILE), BF16),
        in_specs=[VMEM],
        out_specs=VMEM,
        compiler_params=SMALL,
        name="turn",
    )(node_in)
    meta = pl.pallas_call(
        meta_kernel,
        out_shape=jax.ShapeDtypeStruct((relations, TILE), jnp.int32),
        in_specs=[VMEM] * 2 + [SMEM],
        out_specs=VMEM,
        compiler_params=SMALL,
        name="meta",
    )(tile_rows, tile_cols, tile_count.reshape(-1))
    packed = out_grad.T
    pair = jnp.stack([packed, shifted(packed, XHI, 1)])
    grads = [pair] + [shifted(pair, Y, k) for k in (1, 2, 3)]
    inputs = gathered(turned, (XLO, Z))
    tiles_near = shifted(tiles, CORE, 1)
    meta_near = shifted(meta, CORE, 1)

    grad = pl.pallas_call(
        grad_kernel,
        out_shape=jax.ShapeDtypeStruct((d_out // width, width, rows), BF16),
        in_specs=[VMEM] * 4,
        out_specs=VMEM,
        compiler_params=SMALL,
        name="join_grad",
    )(*grads).reshape(d_out, rows)
    grad_near = shifted(grad, CORE, 1)

    mixed, mixed_sent, sums = pl.pallas_call(
        mix_kernel,
        out_shape=(
            jax.ShapeDtypeStruct((8, d_in, TILE), BF16),
            jax.ShapeDtypeStruct((8, d_in, TILE), BF16),
            jax.ShapeDtypeStruct((relations, d_out, 16 * TILE), BF16),
        ),
        in_specs=[SMEM] * 2 + [VMEM] * 3 + [ANY] * 2,
        out_specs=(VMEM,) * 3,
        scratch_shapes=[
            pltpu.SMEM((CAP + UNROLL,), jnp.int32),
            pltpu.VMEM((2, rows // TILE, d_in + d_out, TILE), BF16),
            pltpu.VMEM((16, d_in, TILE), F32),
            pltpu.VMEM((16, d_out, TILE), F32),
            pltpu.VMEM((2, *tiles.shape), BF16),
            pltpu.SemaphoreType.DMA((2, relations)),
        ],
        compiler_params=pltpu.CompilerParams(vmem_limit_bytes=50 * 2**20),
        cost_estimate=BUSY,
        name="mix",
    )(meta, meta_near, grad, grad_near, weights, tiles, tiles_near)
    mixed_met = shifted(mixed_sent, XLO, 1)

    kept, sent = pl.pallas_call(
        weight_kernel,
        out_shape=(
            jax.ShapeDtypeStruct((4, 4, relations, 16, d_out), F32),
            jax.ShapeDtypeStruct((4, 4, relations, 16, d_out), BF16),
        ),
        in_specs=[VMEM] * 2,
        out_specs=(VMEM, VMEM),
        scratch_shapes=[pltpu.VMEM((d_in, 16 * TILE), BF16)],
        compiler_params=pltpu.CompilerParams(vmem_limit_bytes=20 * 2**20),
        cost_estimate=BUSY,
        name="weight_terms",
    )(inputs, sums)

    met = shifted(sent, CORE, 1)
    on_y = [added(kept[k], met[k]) for k in range(4)]
    on_y = [on_y[0]] + [shifted(on_y[k].astype(BF16), Y, k) for k in (1, 2, 3)]
    on_y = added(*on_y)
    on_x = added(on_y[0], *[shifted(on_y[k].astype(BF16), X4, k) for k in (1, 2, 3)])
    on_x, mixed_met = lax.optimization_barrier((on_x, mixed_met))
    on_z = (on_x + swapped(on_x, Z, 1)).astype(BF16)
    mixed = added(mixed, mixed_met).astype(BF16)
    mixed = lax.all_to_all(mixed, Z, 0, 0)
    d_nodes = pl.pallas_call(
        nodes_kernel,
        out_shape=jax.ShapeDtypeStruct(node_in.shape, BF16),
        in_specs=[VMEM],
        out_specs=VMEM,
        compiler_params=SMALL,
        name="nodes",
    )(mixed)

    by = [on_z] + [shifted(on_z, Z, k) for k in (2, 4, 6)]
    total = (added(by[0], by[2]) + added(by[1], by[3])).astype(BF16)
    total = jnp.stack([total] + [shifted(total, X4, k) for k in (1, 2, 3)])
    total = jnp.stack([total] + [shifted(total, Y, k) for k in (1, 2, 3)])
    share = pl.BlockSpec((4, 4, 1, 16, d_out), lambda r: (0, 0, r, 0, 0))
    d_weights = pl.pallas_call(
        join_kernel,
        out_shape=jax.ShapeDtypeStruct((relations, d_in, d_out), F32),
        grid=(relations,),
        in_specs=[share, share],
        out_specs=pl.BlockSpec((1, d_in, d_out), lambda r: (r, 0, 0)),
        compiler_params=SMALL,
        name="join",
    )(total, shifted(total, CORE, 1))
    return d_nodes, d_weights


def solution(mesh):
    finer = Mesh(mesh.devices.reshape(2, 4, 2, 8, 2), (XHI, Y, XLO, Z, CORE))
    in_specs = (
        P(COL, ROW),
        P(ROW + COL, None),
        P(),
        P(None, COL, ROW, None, None, None),
        P(None, COL, ROW, None),
        P(None, COL, ROW, None),
        P(None, COL, ROW),
    )
    out_specs = (P(ROW + COL, None), P())
    return jax.shard_map(body, mesh=finer, in_specs=in_specs, out_specs=out_specs, check_vma=False)
```

```python
import jax
import jax.numpy as jnp
from jax import lax
from jax.experimental import pallas as pl
from jax.experimental.pallas import tpu as pltpu
from jax.sharding import Mesh
from jax.sharding import PartitionSpec as P


XHI, Y, XLO, Z, CORE = "row_0", "row_1", "col_0", "col_1", "col_2"
ROW = (XHI, Y)
COL = (XLO, Z, CORE)
X4 = (XHI, XLO)

UNROLL = 8
CAP = 32
TILE = 128
F32 = jnp.float32
BF16 = jnp.bfloat16
SMEM = pl.BlockSpec(memory_space=pltpu.SMEM)
VMEM = pl.BlockSpec(memory_space=pltpu.VMEM)
ANY = pl.BlockSpec(memory_space=pltpu.HBM)
BUSY = pl.CostEstimate(flops=40 * 10**9, transcendentals=0, bytes_accessed=2**23)
ROOMY = pltpu.CompilerParams(vmem_limit_bytes=26 * 2**20)
SMALL = pltpu.CompilerParams(vmem_limit_bytes=8 * 2**20)


def shifted(value, axis, step):
    n = lax.axis_size(axis)
    return lax.ppermute(value, axis, [(i, (i + step) % n) for i in range(n)])


def gathered(value, axes):
    copies = jnp.broadcast_to(value[None], (lax.axis_size(axes), *value.shape))
    return lax.all_to_all(copies, axes, 0, 0)


def swapped(value, axis, step):
    return lax.ppermute(value, axis, [(i, i ^ step) for i in range(lax.axis_size(axis))])


def added(first, *others):
    total = first.astype(F32)
    for other in others:
        total = total + other.astype(F32)
    return total


def columns(core, meta, r, picked, body):
    count = meta[r, 2 * CAP]

    def pick(s, n):
        picked[n] = s
        return n + jnp.where((meta[r, CAP + s] & 1) == core, 1, 0)

    found = lax.fori_loop(0, count, pick, 0)
    for u in range(UNROLL):
        picked[found + u] = 0

    def group(g, carry):
        at = [g * UNROLL + u for u in range(UNROLL)]
        ids = [picked[i] for i in at]
        body([(s, i < found, meta[r, s], meta[r, CAP + s]) for i, s in zip(at, ids)])
        return carry

    lax.fori_loop(0, (found + UNROLL - 1) // UNROLL, group, 0)


def fetches(tiles0, tiles1, tiles, arrived):
    return lambda a, r: pltpu.make_async_copy((tiles0, tiles1)[a].at[r], tiles.at[a, r], arrived.at[a, r])


def masked(tile, keep):
    return jnp.where(keep, tile, jnp.zeros_like(tile))


def turn_kernel(node_in, turned):
    turned[...] = node_in[...].astype(F32).T.astype(BF16)


def meta_kernel(rows, cols, counts, meta):
    for r in range(meta.shape[0]):
        meta[r : r + 1, :CAP] = rows[r, 0]
        meta[r : r + 1, CAP : 2 * CAP] = cols[r, 0]
        meta[r : r + 1, 2 * CAP :] = jnp.full((1, meta.shape[1] - 2 * CAP), counts[r], jnp.int32)


def grad_kernel(g0, g1, g2, g3, grad):
    x_hi, y = lax.axis_index(XHI), lax.axis_index(Y)
    for k, block in enumerate((g0, g1, g2, g3)):
        for a in range(2):
            grad[(x_hi ^ a) * 4 + ((y - k) & 3)] = block[a]


def mix_kernel(
    meta0, meta1, grad0, grad1, weights, tiles0, tiles1, kept, sent, picked, operands, acc, held_tiles, arrived
):
    core, x_lo = lax.axis_index(CORE), lax.axis_index(XLO)
    fetch = fetches(tiles0, tiles1, held_tiles, arrived)
    for r in range(weights.shape[0]):
        for a in range(2):
            fetch(a, r).start()
    acc[...] = jnp.zeros_like(acc)

    def relation(r, carry):
        for a, (meta, grad) in enumerate(((meta0, grad0), (meta1, grad1))):
            mixed = jnp.dot(weights[r], grad[...], preferred_element_type=F32).astype(BF16)
            for k in range(operands.shape[0]):
                operands[k] = mixed[:, TILE * k : TILE * (k + 1)]
            fetch(a, r).wait()

            def group(entries, a=a):
                products = [
                    jnp.dot(operands[row], masked(held_tiles[a, r, s], keep), preferred_element_type=F32)
                    for s, keep, row, col in entries
                ]
                for (s, keep, row, col), product in zip(entries, products):
                    acc[((col >> 4) ^ x_lo) * 8 + ((col >> 1) & 7)] += product

            columns(core, meta, r, picked, group)
        return carry

    lax.fori_loop(0, weights.shape[0], relation, 0)
    kept[...] = acc[:8].astype(BF16)
    sent[...] = acc[8:].astype(BF16)


def own_kernel(meta0, meta1, grad0, grad1, tiles0, tiles1, sums, picked, operands, acc, held_tiles, arrived):
    core = lax.axis_index(CORE)
    fetch = fetches(tiles0, tiles1, held_tiles, arrived)
    for r in range(tiles0.shape[0]):
        for a in range(2):
            fetch(a, r).start()
    for a, grad in enumerate((grad0, grad1)):
        for k in range(operands.shape[1]):
            operands[a, k] = grad[:, TILE * k : TILE * (k + 1)]

    def relation(r, carry):
        acc[...] = jnp.zeros_like(acc)
        for a, meta in enumerate((meta0, meta1)):
            fetch(a, r).wait()

            def group(entries, a=a):
                products = [
                    jnp.dot(operands[a, row], masked(held_tiles[a, r, s], keep), preferred_element_type=F32)
                    for s, keep, row, col in entries
                ]
                for (s, keep, row, col), product in zip(entries, products):
                    acc[col >> 1] += product

            columns(core, meta, r, picked, group)
        for k in range(acc.shape[0]):
            sums[r, :, TILE * k : TILE * (k + 1)] = acc[k].astype(BF16)
        return carry

    lax.fori_loop(0, tiles0.shape[0], relation, 0)


def weight_kernel(inputs, sums, kept, sent, held):
    core, x_hi, y, x_lo = [lax.axis_index(a) for a in (CORE, XHI, Y, XLO)]
    x = x_hi * 2 + x_lo
    for k in range(inputs.shape[0]):
        held[:, TILE * k : TILE * (k + 1)] = inputs[k]
    for r in range(sums.shape[0]):
        terms = lax.dot_general(held[...], sums[r], (((1,), (1,)), ((), ())), preferred_element_type=F32)
        half = terms.shape[0] // 2
        low, high = terms[:half], terms[half:]
        mine = jnp.where(core == 0, low, high)
        theirs = jnp.where(core == 0, high, low).astype(BF16)
        for yb in range(4):
            for xb in range(4):
                d = (yb * 4 + xb) * 16
                kept[(yb - y) & 3, (xb - x) & 3, r] = mine[d : d + 16]
                sent[(yb - y) & 3, (xb - x) & 3, r] = theirs[d : d + 16]


def nodes_kernel(parts, out):
    total = parts[0].astype(F32)
    for k in range(1, parts.shape[0]):
        total += parts[k].astype(F32)
    out[...] = total.T.astype(BF16)


def join_kernel(own, other, out):
    core, x_hi, y, x_lo = [lax.axis_index(a) for a in (CORE, XHI, Y, XLO)]
    x = x_hi * 2 + x_lo
    for a, block in enumerate((own, other)):
        for ky in range(4):
            for kx in range(4):
                d = ((core ^ a) * 16 + ((y - ky) & 3) * 4 + ((x - kx) & 3)) * 16
                out[0, pl.ds(pl.multiple_of(d, 16), 16), :] = block[ky, kx, 0].astype(F32)


def body(out_grad, node_in, weights, tile_vals, tile_rows, tile_cols, tile_count):
    relations, d_in, d_out = weights.shape
    tiles = tile_vals[:, 0, 0]
    rows, width = out_grad.shape

    turned = pl.pallas_call(
        turn_kernel,
        out_shape=jax.ShapeDtypeStruct((d_in, TILE), BF16),
        in_specs=[VMEM],
        out_specs=VMEM,
        compiler_params=SMALL,
        name="turn",
    )(node_in)
    meta = pl.pallas_call(
        meta_kernel,
        out_shape=jax.ShapeDtypeStruct((relations, TILE), jnp.int32),
        in_specs=[VMEM] * 2 + [SMEM],
        out_specs=VMEM,
        compiler_params=SMALL,
        name="meta",
    )(tile_rows, tile_cols, tile_count.reshape(-1))
    packed = out_grad.T
    pair = jnp.stack([packed, shifted(packed, XHI, 1)])
    grads = [pair] + [shifted(pair, Y, k) for k in (1, 2, 3)]
    inputs = gathered(turned, (XLO, Z))
    tiles_near = shifted(tiles, CORE, 1)
    meta_near = shifted(meta, CORE, 1)

    grad = pl.pallas_call(
        grad_kernel,
        out_shape=jax.ShapeDtypeStruct((d_out // width, width, rows), BF16),
        in_specs=[VMEM] * 4,
        out_specs=VMEM,
        compiler_params=SMALL,
        name="join_grad",
    )(*grads).reshape(d_out, rows)
    grad_near = shifted(grad, CORE, 1)

    tile_scratch = [
        pltpu.VMEM((2, *tiles.shape), BF16),
        pltpu.SemaphoreType.DMA((2, relations)),
    ]
    mixed, mixed_sent = pl.pallas_call(
        mix_kernel,
        out_shape=(
            jax.ShapeDtypeStruct((8, d_in, TILE), BF16),
            jax.ShapeDtypeStruct((8, d_in, TILE), BF16),
        ),
        in_specs=[SMEM] * 2 + [VMEM] * 3 + [ANY] * 2,
        out_specs=(VMEM, VMEM),
        scratch_shapes=[
            pltpu.SMEM((CAP + UNROLL,), jnp.int32),
            pltpu.VMEM((rows // TILE, d_in, TILE), BF16),
            pltpu.VMEM((16, d_in, TILE), F32),
            *tile_scratch,
        ],
        compiler_params=ROOMY,
        cost_estimate=BUSY,
        name="mix",
    )(meta, meta_near, grad, grad_near, weights, tiles, tiles_near)
    sums = pl.pallas_call(
        own_kernel,
        out_shape=jax.ShapeDtypeStruct((relations, d_out, 16 * TILE), BF16),
        in_specs=[SMEM] * 2 + [VMEM] * 2 + [ANY] * 2,
        out_specs=VMEM,
        scratch_shapes=[
            pltpu.SMEM((CAP + UNROLL,), jnp.int32),
            pltpu.VMEM((2, rows // TILE, d_out, TILE), BF16),
            pltpu.VMEM((16, d_out, TILE), F32),
            *tile_scratch,
        ],
        compiler_params=ROOMY,
        cost_estimate=BUSY,
        name="own",
    )(meta, meta_near, grad, grad_near, tiles, tiles_near)

    mixed_met = shifted(mixed_sent, XLO, 1)

    kept, sent = pl.pallas_call(
        weight_kernel,
        out_shape=(
            jax.ShapeDtypeStruct((4, 4, relations, 16, d_out), F32),
            jax.ShapeDtypeStruct((4, 4, relations, 16, d_out), BF16),
        ),
        in_specs=[VMEM] * 2,
        out_specs=(VMEM, VMEM),
        scratch_shapes=[pltpu.VMEM((d_in, 16 * TILE), BF16)],
        compiler_params=pltpu.CompilerParams(vmem_limit_bytes=20 * 2**20),
        cost_estimate=BUSY,
        name="weight_terms",
    )(inputs, sums)

    met = shifted(sent, CORE, 1)
    on_y = [added(kept[k], met[k]) for k in range(4)]
    on_y = [on_y[0]] + [shifted(on_y[k].astype(BF16), Y, k) for k in (1, 2, 3)]
    on_y = added(*on_y)
    on_x = added(on_y[0], *[shifted(on_y[k].astype(BF16), X4, k) for k in (1, 2, 3)])
    on_x, mixed_met = lax.optimization_barrier((on_x, mixed_met))
    on_z = (on_x + swapped(on_x, Z, 1)).astype(BF16)
    mixed = added(mixed, mixed_met).astype(BF16)
    mixed = lax.all_to_all(mixed, Z, 0, 0)
    d_nodes = pl.pallas_call(
        nodes_kernel,
        out_shape=jax.ShapeDtypeStruct(node_in.shape, BF16),
        in_specs=[VMEM],
        out_specs=VMEM,
        compiler_params=SMALL,
        name="nodes",
    )(mixed)

    by = [on_z] + [shifted(on_z, Z, k) for k in (2, 4, 6)]
    total = (added(by[0], by[2]) + added(by[1], by[3])).astype(BF16)
    total = jnp.stack([total] + [shifted(total, X4, k) for k in (1, 2, 3)])
    total = jnp.stack([total] + [shifted(total, Y, k) for k in (1, 2, 3)])
    share = pl.BlockSpec((4, 4, 1, 16, d_out), lambda r: (0, 0, r, 0, 0))
    d_weights = pl.pallas_call(
        join_kernel,
        out_shape=jax.ShapeDtypeStruct((relations, d_in, d_out), F32),
        grid=(relations,),
        in_specs=[share, share],
        out_specs=pl.BlockSpec((1, d_in, d_out), lambda r: (r, 0, 0)),
        compiler_params=SMALL,
        name="join",
    )(total, shifted(total, CORE, 1))
    return d_nodes, d_weights


def solution(mesh):
    finer = Mesh(mesh.devices.reshape(2, 4, 2, 8, 2), (XHI, Y, XLO, Z, CORE))
    in_specs = (
        P(COL, ROW),
        P(ROW + COL, None),
        P(),
        P(None, COL, ROW, None, None, None),
        P(None, COL, ROW, None),
        P(None, COL, ROW, None),
        P(None, COL, ROW),
    )
    out_specs = (P(ROW + COL, None), P())
    return jax.shard_map(body, mesh=finer, in_specs=in_specs, out_specs=out_specs, check_vma=False)
```

```python
import jax
import jax.numpy as jnp
from jax import lax
from jax.experimental import pallas as pl
from jax.experimental.pallas import tpu as pltpu
from jax.sharding import Mesh
from jax.sharding import PartitionSpec as P


XHI, Y, XLO, Z, CORE = "row_0", "row_1", "col_0", "col_1", "col_2"
ROW = (XHI, Y)
COL = (XLO, Z, CORE)
X4 = (XHI, XLO)


UNROLL = 8
CAP = 32
TILE = 128
F32 = jnp.float32
BF16 = jnp.bfloat16
SMEM = pl.BlockSpec(memory_space=pltpu.SMEM)
VMEM = pl.BlockSpec(memory_space=pltpu.VMEM)
ANY = pl.BlockSpec(memory_space=pltpu.HBM)
BUSY = pl.CostEstimate(flops=40 * 10**9, transcendentals=0, bytes_accessed=2**23)
ROOMY = pltpu.CompilerParams(vmem_limit_bytes=26 * 2**20)
SMALL = pltpu.CompilerParams(vmem_limit_bytes=8 * 2**20)


def shifted(value, axis, step):
    n = lax.axis_size(axis)
    return lax.ppermute(value, axis, [(i, (i + step) % n) for i in range(n)])


def swapped(value, axis, step):
    return lax.ppermute(value, axis, [(i, i ^ step) for i in range(lax.axis_size(axis))])


def added(first, *others):
    total = first.astype(F32)
    for other in others:
        total = total + other.astype(F32)
    return total


def columns(core, meta, r, picked, body):
    count = meta[r, 2 * CAP]

    def pick(s, n):
        picked[n] = s
        return n + jnp.where((meta[r, CAP + s] & 1) == core, 1, 0)

    found = lax.fori_loop(0, count, pick, 0)
    for u in range(UNROLL):
        picked[found + u] = 0

    def group(g, carry):
        at = [g * UNROLL + u for u in range(UNROLL)]
        ids = [picked[i] for i in at]
        body([(s, i < found, meta[r, s], meta[r, CAP + s]) for i, s in zip(at, ids)])
        return carry

    lax.fori_loop(0, (found + UNROLL - 1) // UNROLL, group, 0)


def fetches(tiles0, tiles1, tiles, arrived):
    return lambda a, r: pltpu.make_async_copy((tiles0, tiles1)[a].at[r], tiles.at[a, r], arrived.at[a, r])


def masked(tile, keep):
    return jnp.where(keep, tile, jnp.zeros_like(tile))


def turn_kernel(node_in, turned):
    turned[...] = node_in[...].astype(F32).T.astype(BF16)


def meta_kernel(rows, cols, counts, meta):
    for r in range(meta.shape[0]):
        meta[r : r + 1, :CAP] = rows[r, 0]
        meta[r : r + 1, CAP : 2 * CAP] = cols[r, 0]
        meta[r : r + 1, 2 * CAP :] = jnp.full((1, meta.shape[1] - 2 * CAP), counts[r], jnp.int32)


def grad_kernel(g0, g1, g2, g3, grad):
    x_hi, y = lax.axis_index(XHI), lax.axis_index(Y)
    for k, block in enumerate((g0, g1, g2, g3)):
        for a in range(2):
            grad[(x_hi ^ a) * 4 + ((y - k) & 3)] = block[a]


def mix_kernel(
    meta0, meta1, grad0, grad1, weights, tiles0, tiles1, kept, sent, picked, operands, acc, held_tiles, arrived
):
    core, x_lo = lax.axis_index(CORE), lax.axis_index(XLO)
    fetch = fetches(tiles0, tiles1, held_tiles, arrived)
    for r in range(weights.shape[0]):
        for a in range(2):
            fetch(a, r).start()
    acc[...] = jnp.zeros_like(acc)

    def relation(r, carry):
        for a, (meta, grad) in enumerate(((meta0, grad0), (meta1, grad1))):
            mixed = jnp.dot(weights[r], grad[...], preferred_element_type=F32).astype(BF16)
            for k in range(operands.shape[0]):
                operands[k] = mixed[:, TILE * k : TILE * (k + 1)]
            fetch(a, r).wait()

            def group(entries, a=a):
                products = [
                    jnp.dot(operands[row], masked(held_tiles[a, r, s], keep), preferred_element_type=F32)
                    for s, keep, row, col in entries
                ]
                for (s, keep, row, col), product in zip(entries, products):
                    acc[((col >> 4) ^ x_lo) * 8 + ((col >> 1) & 7)] += product

            columns(core, meta, r, picked, group)
        return carry

    lax.fori_loop(0, weights.shape[0], relation, 0)
    kept[...] = acc[:8].astype(BF16)
    sent[...] = acc[8:].astype(BF16)


def own_kernel(meta0, meta1, grad0, grad1, tiles0, tiles1, sums, picked, operands, acc, held_tiles, arrived):
    core = lax.axis_index(CORE)
    fetch = fetches(tiles0, tiles1, held_tiles, arrived)
    for r in range(tiles0.shape[0]):
        for a in range(2):
            fetch(a, r).start()
    for a, grad in enumerate((grad0, grad1)):
        for k in range(operands.shape[1]):
            operands[a, k] = grad[:, TILE * k : TILE * (k + 1)]

    def relation(r, carry):
        acc[...] = jnp.zeros_like(acc)
        for a, meta in enumerate((meta0, meta1)):
            fetch(a, r).wait()

            def group(entries, a=a):
                products = [
                    jnp.dot(operands[a, row], masked(held_tiles[a, r, s], keep), preferred_element_type=F32)
                    for s, keep, row, col in entries
                ]
                for (s, keep, row, col), product in zip(entries, products):
                    acc[col >> 1] += product

            columns(core, meta, r, picked, group)
        for k in range(acc.shape[0]):
            sums[r, :, TILE * k : TILE * (k + 1)] = acc[k].astype(BF16)
        return carry

    lax.fori_loop(0, tiles0.shape[0], relation, 0)


def weight_kernel(*refs):
    parts, (sums, kept, sent, inputs, held) = refs[:8], refs[8:]
    core, x_hi, y, x_lo, z = [lax.axis_index(a) for a in (CORE, XHI, Y, XLO, Z)]
    for k, part in enumerate(parts):
        inputs[2 * k] = part[0]
        inputs[2 * k + 1] = part[1]
    x = x_hi * 2 + x_lo
    for k in range(inputs.shape[0]):
        held[:, TILE * k : TILE * (k + 1)] = inputs[((z - (k & 7)) & 7) * 2 + ((k >> 3) ^ x_lo)]
    for r in range(sums.shape[0]):
        terms = lax.dot_general(held[...], sums[r], (((1,), (1,)), ((), ())), preferred_element_type=F32)
        half = terms.shape[0] // 2
        low, high = terms[:half], terms[half:]
        mine = jnp.where(core == 0, low, high)
        theirs = jnp.where(core == 0, high, low).astype(BF16)
        for yb in range(4):
            for xb in range(4):
                d = (yb * 4 + xb) * 16
                kept[(yb - y) & 3, (xb - x) & 3, r] = mine[d : d + 16]
                sent[(yb - y) & 3, (xb - x) & 3, r] = theirs[d : d + 16]


def nodes_kernel(parts, out):
    total = parts[0].astype(F32)
    for k in range(1, parts.shape[0]):
        total += parts[k].astype(F32)
    out[...] = total.T.astype(BF16)


def join_kernel(own, other, out):
    core, x_hi, y, x_lo = [lax.axis_index(a) for a in (CORE, XHI, Y, XLO)]
    x = x_hi * 2 + x_lo
    for a, block in enumerate((own, other)):
        for ky in range(4):
            for kx in range(4):
                d = ((core ^ a) * 16 + ((y - ky) & 3) * 4 + ((x - kx) & 3)) * 16
                out[0, pl.ds(pl.multiple_of(d, 16), 16), :] = block[ky, kx, 0].astype(F32)


def body(out_grad, node_in, weights, tile_vals, tile_rows, tile_cols, tile_count):
    relations, d_in, d_out = weights.shape
    tiles = tile_vals[:, 0, 0]
    rows, width = out_grad.shape

    turned = pl.pallas_call(
        turn_kernel,
        out_shape=jax.ShapeDtypeStruct((d_in, TILE), BF16),
        in_specs=[VMEM],
        out_specs=VMEM,
        compiler_params=SMALL,
        name="turn",
    )(node_in)
    meta = pl.pallas_call(
        meta_kernel,
        out_shape=jax.ShapeDtypeStruct((relations, TILE), jnp.int32),
        in_specs=[VMEM] * 2 + [SMEM],
        out_specs=VMEM,
        compiler_params=SMALL,
        name="meta",
    )(tile_rows, tile_cols, tile_count.reshape(-1))
    packed = out_grad.T
    pair = jnp.stack([packed, shifted(packed, XHI, 1)])
    grads = [pair] + [shifted(pair, Y, k) for k in (1, 2, 3)]
    near = jnp.stack([turned, shifted(turned, XLO, 1)])
    parts = {0: near}
    for k in (3, -3, 2, -2, 1, -1):
        parts[k % 8] = shifted(near, Z, k)
    parts[4] = shifted(parts[3], Z, 1)
    tiles_near = shifted(tiles, CORE, 1)
    meta_near = shifted(meta, CORE, 1)

    grad = pl.pallas_call(
        grad_kernel,
        out_shape=jax.ShapeDtypeStruct((d_out // width, width, rows), BF16),
        in_specs=[VMEM] * 4,
        out_specs=VMEM,
        compiler_params=SMALL,
        name="join_grad",
    )(*grads).reshape(d_out, rows)
    grad_near = shifted(grad, CORE, 1)

    tile_scratch = [
        pltpu.VMEM((2, *tiles.shape), BF16),
        pltpu.SemaphoreType.DMA((2, relations)),
    ]
    mixed, mixed_sent = pl.pallas_call(
        mix_kernel,
        out_shape=(
            jax.ShapeDtypeStruct((8, d_in, TILE), BF16),
            jax.ShapeDtypeStruct((8, d_in, TILE), BF16),
        ),
        in_specs=[SMEM] * 2 + [VMEM] * 3 + [ANY] * 2,
        out_specs=(VMEM, VMEM),
        scratch_shapes=[
            pltpu.SMEM((CAP + UNROLL,), jnp.int32),
            pltpu.VMEM((rows // TILE, d_in, TILE), BF16),
            pltpu.VMEM((16, d_in, TILE), F32),
            *tile_scratch,
        ],
        compiler_params=ROOMY,
        cost_estimate=BUSY,
        name="mix",
    )(meta, meta_near, grad, grad_near, weights, tiles, tiles_near)
    sums = pl.pallas_call(
        own_kernel,
        out_shape=jax.ShapeDtypeStruct((relations, d_out, 16 * TILE), BF16),
        in_specs=[SMEM] * 2 + [VMEM] * 2 + [ANY] * 2,
        out_specs=VMEM,
        scratch_shapes=[
            pltpu.SMEM((CAP + UNROLL,), jnp.int32),
            pltpu.VMEM((2, rows // TILE, d_out, TILE), BF16),
            pltpu.VMEM((16, d_out, TILE), F32),
            *tile_scratch,
        ],
        compiler_params=ROOMY,
        cost_estimate=BUSY,
        name="own",
    )(meta, meta_near, grad, grad_near, tiles, tiles_near)

    mixed_met = shifted(mixed_sent, XLO, 1)

    kept, sent = pl.pallas_call(
        weight_kernel,
        out_shape=(
            jax.ShapeDtypeStruct((4, 4, relations, 16, d_out), F32),
            jax.ShapeDtypeStruct((4, 4, relations, 16, d_out), BF16),
        ),
        in_specs=[VMEM] * 9,
        out_specs=(VMEM, VMEM),
        scratch_shapes=[pltpu.VMEM((16, d_in, TILE), BF16), pltpu.VMEM((d_in, 16 * TILE), BF16)],
        compiler_params=pltpu.CompilerParams(vmem_limit_bytes=20 * 2**20),
        cost_estimate=BUSY,
        name="weight_terms",
    )(*[parts[k] for k in range(8)], sums)

    met = shifted(sent, CORE, 1)
    on_y = [added(kept[k], met[k]) for k in range(4)]
    on_y = [on_y[0]] + [shifted(on_y[k].astype(BF16), Y, k) for k in (1, 2, 3)]
    on_y = added(*on_y)
    on_x = added(on_y[0], *[shifted(on_y[k].astype(BF16), X4, k) for k in (1, 2, 3)])
    on_x, mixed_met = lax.optimization_barrier((on_x, mixed_met))
    on_z = (on_x + swapped(on_x, Z, 1)).astype(BF16)
    mixed = added(mixed, mixed_met).astype(BF16)
    mixed = lax.all_to_all(mixed, Z, 0, 0)
    d_nodes = pl.pallas_call(
        nodes_kernel,
        out_shape=jax.ShapeDtypeStruct(node_in.shape, BF16),
        in_specs=[VMEM],
        out_specs=VMEM,
        compiler_params=SMALL,
        name="nodes",
    )(mixed)

    by = [on_z] + [shifted(on_z, Z, k) for k in (2, 4, 6)]
    total = (added(by[0], by[2]) + added(by[1], by[3])).astype(BF16)
    total = jnp.stack([total] + [shifted(total, X4, k) for k in (1, 2, 3)])
    total = jnp.stack([total] + [shifted(total, Y, k) for k in (1, 2, 3)])
    share = pl.BlockSpec((4, 4, 1, 16, d_out), lambda r: (0, 0, r, 0, 0))
    d_weights = pl.pallas_call(
        join_kernel,
        out_shape=jax.ShapeDtypeStruct((relations, d_in, d_out), F32),
        grid=(relations,),
        in_specs=[share, share],
        out_specs=pl.BlockSpec((1, d_in, d_out), lambda r: (r, 0, 0)),
        compiler_params=SMALL,
        name="join",
    )(total, shifted(total, CORE, 1))
    return d_nodes, d_weights


def solution(mesh):
    finer = Mesh(mesh.devices.reshape(2, 4, 2, 8, 2), (XHI, Y, XLO, Z, CORE))
    in_specs = (
        P(COL, ROW),
        P(ROW + COL, None),
        P(),
        P(None, COL, ROW, None, None, None),
        P(None, COL, ROW, None),
        P(None, COL, ROW, None),
        P(None, COL, ROW),
    )
    out_specs = (P(ROW + COL, None), P())
    return jax.shard_map(body, mesh=finer, in_specs=in_specs, out_specs=out_specs, check_vma=False)
```
